256 devices in a mesh: tracts: 2 (over y), sky: 32 (over z, core), depth: 4 (over x).
Axes of the slice: x: 4, y: 2, z: 16, core: 2. Of those that a mesh axis runs over, the one named last changes fastest.
The devices are a block of a 4x16x16 slice.
Arguments:
- visit_tiles: bfloat16 [1024, 32, 64, 512], P(('tracts', 'sky', 'depth')), parts along dimension 0, may hold values from -6 to 6
- warp_matrix: bfloat16 [1024, 512, 512], P(('tracts', 'sky', 'depth')), parts along dimension 0, may hold values from -0.25 to 0.25
- flux_scale: float32 [1024], P(('tracts', 'sky', 'depth')), parts along dimension 0, may hold values from 0.3 to 3
- patch_lists: int32 [1024, 32], P(('tracts', 'sky', 'depth')), parts along dimension 0, may hold values from 0 to 127, all different within a row; in each aligned block of 4 rows (0 to 3, 4 to 7, ...) at most 2 rows name the same one
- clip_bits: int32 [1024, 32, 4, 512], P(('tracts', 'sky', 'depth')), parts along dimension 0, may hold values from -2147483648 to 2147483647, as said below
Outputs:
- coadd_mean: float32 [2, 256, 64, 512], P(None, ('tracts', 'sky'), 'depth'), parts along dimension 1
- coadd_var: float32 [2, 256, 64, 512], P(None, ('tracts', 'sky'), 'depth'), parts along dimension 1
The draws below stay inside these ranges and needn't reach their ends.
There are 2 independent parts, one for each index of `tracts`. The reference program is written for one: setup_inputs(seed, part) draws one part's arguments, and reference() takes and returns one part's arrays. A program takes and returns all parts, laid end to end along the dimension named above; each array names one. Nothing has to cross between parts.
Inputs may be any that keep to these rules, and one draw needn't show every extreme that they name: `patch_lists`: row v names the 32 different patches of visit v's blocks. In the rows of one device no patch is named more than 2 times, a bound that some block reaches there; every patch is named by some row. Bit 16 t + j of clip_bits[v, k, g, c] is 1 when clip pass t (t = 0 or 1) keeps the sample of visit v's block k at row 16 g + j, column c.
All inputs are finite; a program needn't handle non-finite values.
Results may differ from the reference program's by a relative error of at most 0.0029.
Values may be sent and summed in bfloat16 or wider, within the bound.
A program may use at most 128 MiB of HBM per device.

```python
import math
import jax
import jax.numpy as jnp
import numpy as np
from jax import lax

COLUMNS = 512
ROWS = 64
VISITS_DEV = 4
CAPACITY = 2
PATCHES = 128
INTERSECTIONS = 32
VISITS = 512


def draw_clip_bits(key, part):
    word_shape = (VISITS, INTERSECTIONS, ROWS // 16, COLUMNS)

    def add_bit(position, packed):
        level = jax.random.randint(jax.random.fold_in(key, position + 7), word_shape, 0, 20, dtype=jnp.int32)
        limit = jnp.where(position < 16, 18, 17)
        kept = (level < limit).astype(jnp.int32)
        return jnp.bitwise_or(packed, jnp.left_shift(kept, position))
    return lax.fori_loop(0, 32, add_bit, jnp.zeros(word_shape, jnp.int32))


def levels(own_key, dims, shards, low, top_value):
    loudness = 1.0
    for dim, parts in shards:
        heights = jax.random.uniform(jax.random.fold_in(jax.random.fold_in(own_key, 6), dim), (parts,), jnp.float32, low / len(shards), top_value / len(shards))
        loudness = loudness * jnp.repeat(jnp.exp(heights), dims[dim] // parts).reshape((-1,) + (1,) * (len(dims) - 1 - dim))
    return loudness


def routed_block(rng, own, number, rows, amount, top, most, lean):
    sequence = jax.random.permutation(rng, amount)
    crowded, common = load_shares(amount, rows * top, most, lean, True), load_shares(amount, rows * top, most, lean, False)
    places = jnp.arange(amount)

    def named(tallies, turn):
        used = int((tallies > 0).sum())
        fixed = max(1, used // 4)
        passed = fixed + (places - fixed + turn * (used - fixed)) % max(1, amount - fixed)
        return jnp.zeros((amount,), jnp.int32).at[sequence[jnp.where(places < fixed, places, passed)]].set(jnp.asarray(tallies, jnp.int32))

    tallies = jnp.where(number % 4 == 0, named(crowded, number // 4), named(common, number - number // 4 - 1))
    mixed = jax.random.permutation(jax.random.fold_in(own, 3), amount)
    giver, receiver = mixed[0:amount // 2 * 2:2], mixed[1:amount // 2 * 2:2]
    room = jnp.minimum(tallies[giver] - 1, most - tallies[receiver]) // 2
    room = jnp.where((giver == sequence[0]) | (receiver == sequence[0]) | (tallies[receiver] == 0), 0, jnp.maximum(room, 0))
    passed = jax.random.randint(jax.random.fold_in(own, 4), (amount // 2,), 0, 1 << 20) % (room + 1)
    tallies = tallies.at[giver].add(-passed).at[receiver].add(passed)
    members = jnp.searchsorted(jnp.cumsum(tallies), jnp.arange(rows * top), side="right").astype(jnp.int32)
    listing = members.reshape(top, rows).T
    listing = listing[jax.random.permutation(jax.random.fold_in(own, 1), rows)]
    turn = jax.random.randint(jax.random.fold_in(own, 2), (rows, 1), 0, top)
    return jnp.take_along_axis(listing, (jnp.arange(top)[None, :] + turn) % top, axis=1)


def load_shares(count, total, most, lean, full):
    weights = [(1 << 20) // math.isqrt(grade ** lean) + 1 for grade in range(1, count + 1)]
    largest = most if full else min(most, max(-(-total // count), total * weights[0] // sum(weights)))
    least = 1 if total - largest >= count - 1 else 0
    counts, surplus = [largest] + [least] * (count - 1), total - largest - least * (count - 1)
    while surplus > 0:
        candidates = [i for i in range(1, count) if counts[i] < largest] or [i for i in range(1, count) if counts[i] < most]
        mass, remaining = sum([weights[i] for i in candidates]), surplus
        for i in candidates:
            extra = min(most - counts[i], max(1, remaining * weights[i] // mass), surplus)
            counts[i] = counts[i] + extra
            surplus = surplus - extra
    return np.array(counts)


def scatter_about(rng, extent, deviation, reach, cuts=(), held_as=jnp.bfloat16):
    entries = jax.random.normal(rng, extent, jnp.float32) * deviation
    if len(cuts) > 0:
        entries = levels(rng, extent, cuts, -0.22, 0.18) * entries
    return jnp.clip(entries, min=-reach, max=reach).astype(held_as)


def setup_inputs(seed: int = 0, part: int = 0) -> dict:
    key_list = jax.random.split(jax.random.key(seed), 6)
    part_splits = jax.random.split(jax.random.fold_in(key_list[5], part), 6)
    visit_tiles = scatter_about(part_splits[0], (VISITS, INTERSECTIONS, ROWS, COLUMNS), 1.0, 6.0, ((0, 128),))
    warp_matrix = scatter_about(part_splits[1], (VISITS, COLUMNS, COLUMNS), COLUMNS ** -0.5, 0.25, ((0, 128),))
    flux_scale = jnp.clip(jnp.exp(math.log(3.0) - 2.3025851 * jax.random.uniform(part_splits[2], (VISITS,), jnp.float32) ** levels(part_splits[2], (VISITS,), ((0, 128),), -0.2, 0.2)), 0.3, 3.0)
    patch_lists_keys = jax.random.split(jax.random.fold_in(part_splits[3], 1), VISITS // VISITS_DEV)
    patch_lists_turns = jax.random.permutation(jax.random.fold_in(part_splits[3], 3), VISITS // VISITS_DEV)
    patch_lists = jax.vmap(lambda own, number: routed_block(jax.random.fold_in(part_splits[3], 2), own, number, VISITS_DEV, PATCHES, INTERSECTIONS, CAPACITY, 2))(patch_lists_keys, patch_lists_turns).reshape((VISITS, INTERSECTIONS))
    clip_bits = draw_clip_bits(jax.random.fold_in(jax.random.fold_in(key_list[5], part), 71), part)
    return {"visit_tiles": visit_tiles, "warp_matrix": warp_matrix, "flux_scale": flux_scale, "patch_lists": patch_lists, "clip_bits": clip_bits}


def unpack_keep(packed, offset):
    positions = jnp.arange(16, dtype=jnp.int32) + offset
    bit_flags = jnp.bitwise_and(jnp.right_shift(packed[..., None, :], positions[:, None]), 1)
    target_shape = packed.shape[:-2] + (packed.shape[-2] * 16, packed.shape[-1])
    return bit_flags.reshape(target_shape).astype(jnp.float32)


def finish(count_first, sum_first, square_first, count_both, shift_sum, shift_square):
    first_mean = sum_first / jnp.maximum(count_first, 1.0)
    first_var = (square_first - sum_first * first_mean) / jnp.maximum(count_first - 1.0, 1.0)
    final_mean = first_mean + shift_sum / jnp.maximum(count_both, 1.0)
    final_var = (shift_square - shift_sum * shift_sum / jnp.maximum(count_both, 1.0)) / jnp.maximum(count_both - 1.0, 1.0)
    return jnp.stack([first_mean, final_mean]), jnp.stack([first_var, final_var])


def reference(visit_tiles, warp_matrix, flux_scale, patch_lists, clip_bits):
    def warp_one(member):
        tile_block, matrix, factor = member
        product = jnp.dot(tile_block.reshape(INTERSECTIONS * ROWS, COLUMNS), matrix, preferred_element_type=jnp.float32)
        return (product * factor).astype(jnp.bfloat16).reshape(INTERSECTIONS, ROWS, COLUMNS)

    warped = lax.map(warp_one, (visit_tiles, warp_matrix, flux_scale))
    initial = jnp.zeros((PATCHES, ROWS, COLUMNS), jnp.float32)

    def first_step(state_sums, member):
        counted, totals, squares = state_sums
        warped_rows, packed, targets = member
        samples = warped_rows.astype(jnp.float32)
        keep_mask = unpack_keep(packed, 0)
        return (counted.at[targets].add(keep_mask), totals.at[targets].add(keep_mask * samples),
                squares.at[targets].add(keep_mask * samples * samples)), None

    (count_first, sum_first, square_first), _ = lax.scan(first_step, (initial, initial, initial), (warped, clip_bits, patch_lists))
    first_mean = sum_first / jnp.maximum(count_first, 1.0)

    def second_step(state_sums, member):
        counted, totals, squares = state_sums
        warped_rows, packed, targets = member
        samples = warped_rows.astype(jnp.float32)
        keep_mask = unpack_keep(packed, 0) * unpack_keep(packed, 16)
        centred = samples - first_mean[targets]
        return (counted.at[targets].add(keep_mask), totals.at[targets].add(keep_mask * centred),
                squares.at[targets].add(keep_mask * centred * centred)), None

    (count_both, shift_sum, shift_square), _ = lax.scan(second_step, (initial, initial, initial), (warped, clip_bits, patch_lists))
    return finish(count_first, sum_first, square_first, count_both, shift_sum, shift_square)
```

```python
import functools

import jax
import jax.numpy as jnp
from jax import lax
from jax.experimental import pallas as pl
from jax.experimental.pallas import tpu as pltpu
from jax.sharding import PartitionSpec as P

PATCH_DEV = 4
CAPACITY = 2
CORES = 2
LANES = 128
FIELDS = 5
COUNT_UNIT = 4096.0
MESH = pl.DeviceIdType.MESH


def kernel_body(
    dims,
    tiles_hbm,
    warp_hbm,
    flux,
    bits_hbm,
    table_hbm,
    mean_out,
    var_out,
    tiles,
    warp,
    table_v,
    table,
    *refs,
):
    visits, blocks, rows, columns, xs, zs = dims
    entries = visits * blocks
    share = rows // xs
    chunks = columns // LANES
    half = zs // 2
    x_send, x_recv, bits = refs[:chunks], refs[chunks : 2 * chunks], refs[2 * chunks : 3 * chunks]
    (
        parts,
        parts_last,
        pair_recv,
        pair_recv_last,
        ring_send,
        ring_recv,
        load_sem,
        table_sem,
        own_sem,
        x_ssem,
        x_rsem,
        bits_ssem,
        bits_rsem,
        pair_ssem,
        pair_rsem,
        ring_ssem,
        ring_rsem,
    ) = refs[3 * chunks :]
    tract = lax.axis_index("tracts")
    sky = lax.axis_index("sky")
    x = lax.axis_index("depth")
    z, core = sky // CORES, lax.rem(sky, CORES)

    def x_peer(dx):
        return lax.rem(x + dx, xs)

    def z_peer(direction):
        step = 1 if direction == 0 else zs - 1
        return (tract, lax.rem(z + step, zs) * CORES + core, x)

    partner = (tract, z * CORES + (1 - core), x)

    barrier = pltpu.get_barrier_semaphore()
    greeted = [(tract, sky, x_peer(dx)) for dx in range(1, xs)]
    greeted += [z_peer(0), z_peer(1), partner]
    for device in greeted:
        pl.semaphore_signal(barrier, inc=1, device_id=device, device_id_type=MESH)

    def load_visit(v):
        return (
            pltpu.make_async_copy(tiles_hbm.at[v], tiles.at[v], load_sem.at[v, 0]),
            pltpu.make_async_copy(warp_hbm.at[v], warp.at[v], load_sem.at[v, 1]),
        )

    for v in range(visits):
        for copy in load_visit(v):
            copy.start()
    for j in range(chunks):
        for s in range(xs):
            x_recv[j][s, entries] = jnp.zeros((share, LANES), jnp.bfloat16)
            bits[j][s, pl.ds(entries, 8), :] = jnp.zeros((8, LANES), jnp.int32)
    pl.semaphore_wait(barrier, len(greeted))

    def table_copy(dx):
        return pltpu.make_async_remote_copy(
            src_ref=table_hbm,
            dst_ref=table_v.at[x],
            send_sem=table_sem.at[0, dx],
            recv_sem=table_sem.at[1, dx],
            device_id=(tract, sky, x_peer(dx)),
            device_id_type=MESH,
        )

    def bits_copy(j, dx):
        return pltpu.make_async_remote_copy(
            src_ref=bits_hbm.at[x_peer(dx), j],
            dst_ref=bits[j].at[x, pl.ds(0, entries)],
            send_sem=bits_ssem.at[j, dx],
            recv_sem=bits_rsem.at[j, dx],
            device_id=(tract, sky, x_peer(dx)),
            device_id_type=MESH,
        )

    def x_copy(j, v, dx):
        part = pl.ds(v * blocks, blocks)
        return pltpu.make_async_remote_copy(
            src_ref=x_send[j].at[x_peer(dx), part],
            dst_ref=x_recv[j].at[x, part],
            send_sem=x_ssem.at[j, v, dx],
            recv_sem=x_rsem.at[j, v, dx],
            device_id=(tract, sky, x_peer(dx)),
            device_id_type=MESH,
        )

    def own_bits(j):
        return pltpu.make_async_copy(
            bits_hbm.at[x, j], bits[j].at[x, pl.ds(0, entries)], own_sem.at[j, 0]
        )

    def own_rows(j):
        return pltpu.make_async_copy(
            x_send[j].at[x], x_recv[j].at[x, pl.ds(0, entries)], own_sem.at[j, 1]
        )

    own_table = pltpu.make_async_copy(table_hbm, table_v.at[x], table_sem.at[0, 0])
    own_table.start()
    for dx in range(1, xs):
        table_copy(dx).start()

    group = 8
    for j in range(chunks):
        own_bits(j).start()
        for dx in range(1, xs):
            bits_copy(j, dx).start()
        for v in range(visits):
            if j == 0:
                for copy in load_visit(v):
                    copy.wait()
            weights = warp[v, :, pl.ds(j * LANES, LANES)]
            scale = flux[v]

            def multiply(n, carry):
                first = pl.multiple_of(n * (group * rows), group * rows)
                product = jnp.dot(
                    tiles[v, pl.ds(first, group * rows), :],
                    weights,
                    preferred_element_type=jnp.float32,
                )
                scaled = (product * scale).astype(jnp.bfloat16)
                scaled = scaled.reshape(group, xs, share, LANES)
                at = pl.ds(v * blocks + n * group, group)
                for d in range(xs):
                    x_send[j][d, at] = scaled[:, d]
                return carry

            lax.fori_loop(0, blocks // group, multiply, 0)
            for dx in range(1, xs):
                x_copy(j, v, dx).start()
        own_rows(j).start()

    own_table.wait()
    for dx in range(1, xs):
        table_copy(dx).wait()
    to_scalar = pltpu.make_async_copy(table_v, table, table_sem.at[1, 0])
    to_scalar.start()
    to_scalar.wait()

    def wait_chunk(j):
        own_bits(j).wait()
        own_rows(j).wait()
        for dx in range(1, xs):
            bits_copy(j, dx).wait()
            for v in range(visits):
                x_copy(j, v, dx).wait()

    row = lax.broadcasted_iota(jnp.int32, (share, LANES), 0)
    mask_first = jnp.left_shift(jnp.int32(1), row)
    mask_both = jnp.bitwise_or(mask_first, jnp.left_shift(jnp.int32(1), row + 16))
    zero = jnp.zeros((share, LANES), jnp.float32)

    def patch_sums(j, patch):
        count, s1, q1, sb, qb = zero, zero, zero, zero, zero
        for s in range(xs):
            for r in range(CAPACITY):
                e = table[s, r, patch]
                sample = x_recv[j][s, e].astype(jnp.float32)
                word = bits[j][s, pl.ds(e, 1), :]
                first = jnp.bitwise_and(word, mask_first) != 0
                both = jnp.bitwise_and(word, mask_both) == mask_both
                kept = jnp.where(first, sample, 0.0)
                s1 = s1 + kept
                q1 = q1 + kept * kept
                kept = jnp.where(both, sample, 0.0)
                sb = sb + kept
                qb = qb + kept * kept
                count = count + jnp.where(
                    both, 1.0 + COUNT_UNIT, jnp.where(first, 1.0, 0.0)
                )
        return count, s1, q1, sb, qb

    def pair_copy(j, k):
        return pltpu.make_async_remote_copy(
            src_ref=parts.at[0],
            dst_ref=pair_recv.at[j, k],
            send_sem=pair_ssem.at[0],
            recv_sem=pair_rsem.at[j, k],
            device_id=partner,
            device_id_type=MESH,
        )

    def pair_copy_last(j):
        return pltpu.make_async_remote_copy(
            src_ref=parts_last.at[0],
            dst_ref=pair_recv_last.at[j],
            send_sem=pair_ssem.at[1],
            recv_sem=pair_rsem.at[j, half],
            device_id=partner,
            device_id_type=MESH,
        )

    def store_sums(dst, at, j, patch):
        for f, value in enumerate(patch_sums(j, patch)):
            dst[at[:-1] + (f, at[-1])] = value

    def partials(j, k):
        def side(w, outer):
            which = lax.rem(core + 1 + w, CORES)

            def one(n, inner):
                direction, i = n // PATCH_DEV, lax.rem(n, PATCH_DEV)
                moved = half + k * (2 * direction - 1)
                base = (lax.rem(z + moved, zs) * CORES + which) * PATCH_DEV
                store_sums(parts, (w, direction, i // 2, lax.rem(i, 2)), j, base + i)
                return inner

            lax.fori_loop(0, 2 * PATCH_DEV, one, 0)

            @pl.when(w == 0)
            def _():
                pair_copy(j, k).start()

            return outer

        lax.fori_loop(0, CORES, side, 0)

    def partials_last(j):
        def side(w, outer):
            base = (z * CORES + lax.rem(core + 1 + w, CORES)) * PATCH_DEV

            def one(i, inner):
                store_sums(parts_last, (w, i // 2, lax.rem(i, 2)), j, base + i)
                return inner

            lax.fori_loop(0, PATCH_DEV, one, 0)

            @pl.when(w == 0)
            def _():
                pair_copy_last(j).start()

            return outer

        lax.fori_loop(0, CORES, side, 0)

    def ring_copy(j, k, direction, h):
        return pltpu.make_async_remote_copy(
            src_ref=ring_send.at[lax.rem(k, 2), direction, h],
            dst_ref=ring_recv.at[j, k, direction, h],
            send_sem=ring_ssem.at[lax.rem(k, 2), direction, h],
            recv_sem=ring_rsem.at[j, k, direction, h],
            device_id=z_peer(direction),
            device_id_type=MESH,
        )

    def starts_at_zero(direction, h):
        return direction == h

    def tick(j, k, stage):
        pair_copy(j, k).wait()
        for h in range(2):
            for direction in range(2):
                if stage == 0 and not starts_at_zero(direction, h):
                    continue
                message = parts[1, direction, h] + pair_recv[j, k, direction, h]
                if stage == 2 or (stage == 1 and starts_at_zero(direction, h)):
                    ring_copy(j, k - 1, direction, h).wait()
                    message = message + ring_recv[j, k - 1, direction, h]
                ring_send[lax.rem(k, 2), direction, h] = message
                ring_copy(j, k, direction, h).start()

    def finish(j):
        pair_copy_last(j).wait()
        lanes = pl.ds(j * LANES, LANES)
        for h in range(2):
            total = parts_last[1, h] + pair_recv_last[j, h]
            for direction in range(2):
                if half > 1 or starts_at_zero(direction, h):
                    ring_copy(j, half - 1, direction, h).wait()
                    total = total + ring_recv[j, half - 1, direction, h]
            packed, s1, q1, sb, qb = (total[f] for f in range(FIELDS))
            count_both = jnp.floor(packed * (1.0 / COUNT_UNIT))
            count_first = packed - count_both * COUNT_UNIT
            first_mean = s1 / jnp.maximum(count_first, 1.0)
            first_var = (q1 - s1 * first_mean) / jnp.maximum(count_first - 1.0, 1.0)
            shift_sum = sb - first_mean * count_both
            shift_square = qb - first_mean * (sb + shift_sum)
            move = shift_sum / jnp.maximum(count_both, 1.0)
            final_var = (shift_square - shift_sum * move) / jnp.maximum(
                count_both - 1.0, 1.0
            )
            at = pl.ds(2 * h, 2)
            mean_out[0, at, :, lanes] = first_mean
            mean_out[1, at, :, lanes] = first_mean + move
            var_out[0, at, :, lanes] = first_var
            var_out[1, at, :, lanes] = final_var

    wait_chunk(0)
    partials(0, 0)

    for j in range(chunks):
        tick(j, 0, 0)
        if j > 0:
            finish(j - 1)
        if half > 1:
            partials(j, 1)
            tick(j, 1, 1)

            def later(k, carry):
                partials(j, k)
                tick(j, k, 2)
                return carry

            lax.fori_loop(2, half, later, 0)
        partials_last(j)
        if j < chunks - 1:
            wait_chunk(j + 1)
            partials(j + 1, 0)
    finish(chunks - 1)


def per_device(visit_tiles, warp_matrix, flux_scale, patch_lists, clip_bits):
    visits, blocks, rows, columns = visit_tiles.shape
    entries = visits * blocks
    xs = lax.axis_size("depth")
    skies = lax.axis_size("sky")
    zs = skies // CORES
    half = zs // 2
    share = rows // xs
    chunks = columns // LANES
    patches = PATCH_DEV * skies

    targets = patch_lists.reshape(entries, 1)
    named = targets == jnp.arange(patches, dtype=jnp.int32)[None, :]
    number = jnp.arange(entries, dtype=jnp.int32)[:, None]
    lowest = jnp.min(jnp.where(named, number, entries), axis=0)
    highest = jnp.max(jnp.where(named, number, -1), axis=0)
    table = jnp.stack([lowest, jnp.where(highest > lowest, highest, entries)])

    bits = clip_bits.reshape(entries, xs, chunks, LANES).transpose(1, 2, 0, 3)
    tiles = visit_tiles.reshape(visits, blocks * rows, columns)

    dims = (visits, blocks, rows, columns, xs, zs)
    out = jax.ShapeDtypeStruct((2, PATCH_DEV, share, columns), jnp.float32)
    any_spec = pl.BlockSpec(memory_space=pl.ANY)
    vmem_spec = pl.BlockSpec(memory_space=pltpu.VMEM)
    dma = pltpu.SemaphoreType.DMA
    message = (FIELDS, 2, share, LANES)
    return pl.pallas_call(
        functools.partial(kernel_body, dims),
        out_shape=(out, out),
        in_specs=[
            any_spec,
            any_spec,
            pl.BlockSpec(memory_space=pltpu.SMEM),
            any_spec,
            any_spec,
        ],
        out_specs=(vmem_spec, vmem_spec),
        scratch_shapes=[
            pltpu.VMEM((visits, blocks * rows, columns), jnp.bfloat16),
            pltpu.VMEM((visits, columns, columns), jnp.bfloat16),
            pltpu.VMEM((xs, CAPACITY, patches), jnp.int32),
            pltpu.SMEM((xs, CAPACITY, patches), jnp.int32),
            *[pltpu.VMEM((xs, entries, share, LANES), jnp.bfloat16)] * chunks,
            *[pltpu.VMEM((xs, entries + 1, share, LANES), jnp.bfloat16)] * chunks,
            *[pltpu.VMEM((xs, entries + 8, LANES), jnp.int32)] * chunks,
            pltpu.VMEM((2, 2, 2) + message, jnp.float32),
            pltpu.VMEM((2, 2) + message, jnp.float32),
            pltpu.VMEM((chunks, half, 2, 2) + message, jnp.float32),
            pltpu.VMEM((chunks, 2) + message, jnp.float32),
            pltpu.VMEM((2, 2, 2) + message, jnp.float32),
            pltpu.VMEM((chunks, half, 2, 2) + message, jnp.float32),
            dma((visits, 2)),
            dma((2, xs)),
            dma((chunks, 2)),
            dma((chunks, visits, xs)),
            dma((chunks, visits, xs)),
            dma((chunks, xs)),
            dma((chunks, xs)),
            dma((2,)),
            dma((chunks, half + 1)),
            dma((2, 2, 2)),
            dma((chunks, half, 2, 2)),
        ],
        compiler_params=pltpu.CompilerParams(
            collective_id=0,
            has_side_effects=True,
            vmem_limit_bytes=66 * 1000 * 1000,
        ),
        name="coadd",
    )(tiles, warp_matrix, flux_scale, bits, table)


def solution(mesh):
    placed = (
        P(("tracts", "sky", "depth"), None, None, None),
        P(("tracts", "sky", "depth"), None, None),
        P(("tracts", "sky", "depth")),
        P(("tracts", "sky", "depth"), None),
        P(("tracts", "sky", "depth"), None, None, None),
    )
    return jax.shard_map(
        per_device,
        mesh=mesh,
        in_specs=placed,
        out_specs=(
            P(None, ("tracts", "sky"), "depth", None),
            P(None, ("tracts", "sky"), "depth", None),
        ),
        check_vma=False,
    )
```

```python
import functools

import jax
import jax.numpy as jnp
from jax import lax
from jax.experimental import pallas as pl
from jax.experimental.pallas import tpu as pltpu
from jax.sharding import PartitionSpec as P

PATCH_DEV = 4
CAPACITY = 2
CORES = 2
LANES = 128
SUBLANES = 8
SUMS = 5
FLOATS = 3
RINGS = 4
COUNT_UNIT = 4096.0
SHIFT_STEPS = 32767.0
RATIO_STEPS = 65535.0
TINY = 1e-37
MESH = pl.DeviceIdType.MESH


def kernel_body(
    dims,
    tiles_hbm,
    warp_hbm,
    flux,
    bits_hbm,
    table_hbm,
    mean_out,
    var_out,
    tiles,
    warp,
    table_v,
    table,
    *refs,
):
    visits, blocks, rows, columns, xs, zs = dims
    entries = visits * blocks
    share = rows // xs
    chunks = columns // LANES
    slabs = share // SUBLANES
    units = chunks * slabs
    half = zs // 2
    rings = min(RINGS, half)
    lead = half // rings
    x_send, x_recv = refs[:units], refs[units : 2 * units]
    bits = refs[2 * units : 2 * units + chunks]
    (
        parts,
        parts_last,
        pair_recv,
        pair_recv_last,
        ring_send,
        ring_recv,
        code_send,
        code_recv,
        load_sem,
        table_sem,
        own_sem,
        x_ssem,
        x_rsem,
        bits_ssem,
        bits_rsem,
        pair_ssem,
        pair_rsem,
        ring_ssem,
        ring_rsem,
    ) = refs[2 * units + chunks :]
    tract = lax.axis_index("tracts")
    sky = lax.axis_index("sky")
    x = lax.axis_index("depth")
    z, core = sky // CORES, lax.rem(sky, CORES)

    def x_peer(dx):
        return lax.rem(x + dx, xs)

    def z_peer(direction):
        step = 1 if direction == 0 else zs - 1
        return (tract, lax.rem(z + step, zs) * CORES + core, x)

    partner = (tract, z * CORES + (1 - core), x)

    barrier = pltpu.get_barrier_semaphore()
    greeted = [(tract, sky, x_peer(dx)) for dx in range(1, xs)]
    greeted += [z_peer(0), z_peer(1), partner]
    for device in greeted:
        pl.semaphore_signal(barrier, inc=1, device_id=device, device_id_type=MESH)

    def load_visit(v):
        return (
            pltpu.make_async_copy(tiles_hbm.at[v], tiles.at[v], load_sem.at[v, 0]),
            pltpu.make_async_copy(warp_hbm.at[v], warp.at[v], load_sem.at[v, 1]),
        )

    for v in range(visits):
        for copy in load_visit(v):
            copy.start()
    for s in range(xs):
        for u in range(units):
            x_recv[u][s, entries] = jnp.zeros((SUBLANES, LANES), jnp.bfloat16)
        for j in range(chunks):
            bits[j][s, pl.ds(entries, 8), :] = jnp.zeros((8, LANES), jnp.int32)
    pl.semaphore_wait(barrier, len(greeted))

    def table_copy(dx):
        return pltpu.make_async_remote_copy(
            src_ref=table_hbm,
            dst_ref=table_v.at[x],
            send_sem=table_sem.at[0, dx],
            recv_sem=table_sem.at[1, dx],
            device_id=(tract, sky, x_peer(dx)),
            device_id_type=MESH,
        )

    def bits_copy(j, dx):
        return pltpu.make_async_remote_copy(
            src_ref=bits_hbm.at[x_peer(dx), j],
            dst_ref=bits[j].at[x, pl.ds(0, entries)],
            send_sem=bits_ssem.at[j, dx],
            recv_sem=bits_rsem.at[j, dx],
            device_id=(tract, sky, x_peer(dx)),
            device_id_type=MESH,
        )

    def x_copies(u, dx):
        pieces = visits if u == 0 else 1
        size = entries // pieces
        return [
            pltpu.make_async_remote_copy(
                src_ref=x_send[u].at[x_peer(dx), pl.ds(n * size, size)],
                dst_ref=x_recv[u].at[x, pl.ds(n * size, size)],
                send_sem=x_ssem.at[u, n, dx],
                recv_sem=x_rsem.at[u, n, dx],
                device_id=(tract, sky, x_peer(dx)),
                device_id_type=MESH,
            )
            for n in range(pieces)
        ]

    def own_bits(j):
        return pltpu.make_async_copy(
            bits_hbm.at[x, j], bits[j].at[x, pl.ds(0, entries)], own_sem.at[units + j]
        )

    def own_rows(u):
        return pltpu.make_async_copy(
            x_send[u].at[x], x_recv[u].at[x, pl.ds(0, entries)], own_sem.at[u]
        )

    own_table = pltpu.make_async_copy(table_hbm, table_v.at[x], table_sem.at[0, 0])
    own_table.start()
    for dx in range(1, xs):
        table_copy(dx).start()

    group = 8
    for j in range(chunks):
        own_bits(j).start()
        for dx in range(1, xs):
            bits_copy(j, dx).start()
        for v in range(visits):
            if j == 0:
                for copy in load_visit(v):
                    copy.wait()
            weights = warp[v, :, pl.ds(j * LANES, LANES)]
            scale = flux[v]

            def multiply(n, carry):
                first = pl.multiple_of(n * (group * rows), group * rows)
                product = jnp.dot(
                    tiles[v, pl.ds(first, group * rows), :],
                    weights,
                    preferred_element_type=jnp.float32,
                )
                scaled = (product * scale).reshape(group, xs, slabs, SUBLANES, LANES)
                at = pl.ds(v * blocks + n * group, group)
                for d in range(xs):
                    for slab in range(slabs):
                        x_send[j * slabs + slab][d, at] = scaled[:, d, slab].astype(
                            jnp.bfloat16
                        )
                return carry

            lax.fori_loop(0, blocks // group, multiply, 0)
            if j == 0:
                for dx in range(1, xs):
                    x_copies(0, dx)[v].start()
        for u in range(j * slabs, (j + 1) * slabs):
            if u > 0:
                for dx in range(1, xs):
                    x_copies(u, dx)[0].start()
            own_rows(u).start()

    own_table.wait()
    for dx in range(1, xs):
        table_copy(dx).wait()
    to_scalar = pltpu.make_async_copy(table_v, table, table_sem.at[1, 0])
    to_scalar.start()
    to_scalar.wait()

    def wait_unit(u):
        if u % slabs == 0:
            own_bits(u // slabs).wait()
            for dx in range(1, xs):
                bits_copy(u // slabs, dx).wait_recv()
        own_rows(u).wait()
        for dx in range(1, xs):
            for copy in x_copies(u, dx):
                copy.wait_recv()

    def wait_unit_sent(u):
        for dx in range(1, xs):
            if u % slabs == 0:
                bits_copy(u // slabs, dx).wait_send()
            for copy in x_copies(u, dx):
                copy.wait_send()

    row = lax.broadcasted_iota(jnp.int32, (SUBLANES, LANES), 0)
    zero = jnp.zeros((SUBLANES, LANES), jnp.float32)

    def patch_sums(u, patch):
        j, slab = u // slabs, u % slabs
        mask_first = jnp.left_shift(jnp.int32(1), row + slab * SUBLANES)
        mask_both = jnp.bitwise_or(
            mask_first, jnp.left_shift(jnp.int32(1), row + (16 + slab * SUBLANES))
        )

        def source(s, sums):
            count, s1, q1, sb, qb = sums
            for r in range(CAPACITY):
                e = table[s, r, patch]
                sample = x_recv[u][s, e].astype(jnp.float32)
                word = bits[j][s, pl.ds(e, 1), :]
                first = jnp.bitwise_and(word, mask_first) != 0
                both = jnp.bitwise_and(word, mask_both) == mask_both
                kept = jnp.where(first, sample, 0.0)
                s1 = s1 + kept
                q1 = q1 + kept * kept
                kept = jnp.where(both, sample, 0.0)
                sb = sb + kept
                qb = qb + kept * kept
                count = count + jnp.where(
                    both, 1.0 + COUNT_UNIT, jnp.where(first, 1.0, 0.0)
                )
            return count, s1, q1, sb, qb

        return lax.fori_loop(0, xs, source, (zero,) * SUMS, unroll=True)

    def ring_slot(u):
        return lax.rem(u, rings)

    def pair_copy(u, k):
        return pltpu.make_async_remote_copy(
            src_ref=parts.at[ring_slot(u), 0],
            dst_ref=pair_recv.at[ring_slot(u), k],
            send_sem=pair_ssem.at[ring_slot(u)],
            recv_sem=pair_rsem.at[ring_slot(u), k],
            device_id=partner,
            device_id_type=MESH,
        )

    def pair_copy_last(u):
        return pltpu.make_async_remote_copy(
            src_ref=parts_last.at[0],
            dst_ref=pair_recv_last.at[ring_slot(u)],
            send_sem=pair_ssem.at[rings],
            recv_sem=pair_rsem.at[ring_slot(u), half],
            device_id=partner,
            device_id_type=MESH,
        )

    def store_group(dst, at, u, group):
        def two(h, carry):
            for q in range(2):
                sums = patch_sums(u, group * PATCH_DEV + 2 * h + q)
                for f, value in enumerate(sums):
                    dst[at + (h, f, q)] = value
            return carry

        lax.fori_loop(0, PATCH_DEV // 2, two, 0, unroll=True)

    def partials(u, k):
        if not (isinstance(k, int) and k == 0):
            pair_copy(u, k - 1).wait_send()
        forth = lax.rem(z + (half - k), zs) * CORES
        back = lax.rem(z + (half + k), zs) * CORES

        def one(n, carry):
            w, direction = jnp.right_shift(n, 1), jnp.bitwise_and(n, 1)
            which = jnp.where(w == 0, 1 - core, core)
            group = jnp.where(direction == 0, forth, back) + which
            store_group(parts, (ring_slot(u), w, direction), u, group)

            @pl.when(n == 1)
            def _():
                pair_copy(u, k).start()

            return carry

        lax.fori_loop(0, 2 * CORES, one, 0)

    def partials_last(u):
        pair_copy(u, half - 1).wait_send()
        if half > 1:
            wait_ring_sent(u, half - 2, half == 2)

        def one(w, carry):
            which = jnp.where(w == 0, 1 - core, core)
            store_group(parts_last, (w,), u, z * CORES + which)

            @pl.when(w == 0)
            def _():
                pair_copy_last(u).start()

            return carry

        lax.fori_loop(0, CORES, one, 0)

    def counts(packed):
        both = jnp.floor(packed * (1.0 / COUNT_UNIT))
        return packed - both * COUNT_UNIT, both

    def encode(packed, s1, q1, sb, qb):
        c1, cb = counts(packed)
        mean = s1 / jnp.maximum(c1, 1.0)
        mean_both = sb / jnp.maximum(cb, 1.0)
        m1 = jnp.maximum(q1 - s1 * mean, 0.0)
        mb = jnp.maximum(qb - sb * mean_both, 0.0)
        unit = lax.rsqrt(jnp.maximum(m1, TINY))
        shift = (mean_both - mean) * jnp.sqrt(cb) * unit
        shift = jnp.clip(shift, -1.0, 1.0) * SHIFT_STEPS
        ratio = jnp.minimum(mb * unit * unit, 1.0) * RATIO_STEPS
        code = jnp.bitwise_or(
            jnp.left_shift(jnp.floor(shift + 0.5).astype(jnp.int32), 16),
            jnp.floor(ratio + 0.5).astype(jnp.int32),
        )
        return (packed, s1, m1), code

    def decode(packed, s1, m1, code):
        c1, cb = counts(packed)
        mean = s1 / jnp.maximum(c1, 1.0)
        shift = jnp.right_shift(code, 16).astype(jnp.float32) * (1.0 / SHIFT_STEPS)
        ratio = jnp.bitwise_and(code, 65535).astype(jnp.float32) * (1.0 / RATIO_STEPS)
        spread = jnp.sqrt(m1) * lax.rsqrt(jnp.maximum(cb, 1.0))
        mean_both = mean + shift * spread
        sb = cb * mean_both
        return packed, s1, m1 + s1 * mean, sb, ratio * m1 + sb * mean_both

    def ring_copies(u, k, direction, h):
        par = ring_slot(u)
        return [
            pltpu.make_async_remote_copy(
                src_ref=send.at[par, lax.rem(k, 2), direction, h],
                dst_ref=recv.at[par, k, direction, h],
                send_sem=ring_ssem.at[par, lax.rem(k, 2), direction, h, kind],
                recv_sem=ring_rsem.at[par, k, direction, h, kind],
                device_id=z_peer(direction),
                device_id_type=MESH,
            )
            for kind, (send, recv) in enumerate(
                ((ring_send, ring_recv), (code_send, code_recv))
            )
        ]

    def wait_ring(u, k, direction, h):
        for copy in ring_copies(u, k, direction, h):
            copy.wait_recv()

    def wait_ring_sent(u, k, outset=False):
        for h in range(2):
            for direction in range(2):
                if not outset or direction == h:
                    for copy in ring_copies(u, k, direction, h):
                        copy.wait_send()

    def received(u, k, direction, h):
        at = (ring_slot(u), k, direction, h)
        return decode(*(ring_recv[at + (f,)] for f in range(FLOATS)), code_recv[at])

    def tick(u, k, stage):
        par = ring_slot(u)
        pair_copy(u, k).wait_recv()
        if stage > 1:

            @pl.when(k > 2)
            def _():
                wait_ring_sent(u, k - 2)

            @pl.when(k == 2)
            def _():
                wait_ring_sent(u, 0, True)

        for h in range(2):
            going = [d for d in range(2) if stage > 0 or d == h]
            coming = [d for d in range(2) if stage > 1 or (stage == 1 and d == h)]
            for direction in coming:
                wait_ring(u, k - 1, direction, h)
            ready = []
            for direction in going:
                sums = [
                    parts[par, 1, direction, h, f] + pair_recv[par, k, direction, h, f]
                    for f in range(SUMS)
                ]
                if direction in coming:
                    earlier = received(u, k - 1, direction, h)
                    sums = [a + b for a, b in zip(sums, earlier)]
                ready.append(encode(*sums))
            for direction, (floats, code) in zip(going, ready):
                for f in range(FLOATS):
                    ring_send[par, lax.rem(k, 2), direction, h, f] = floats[f]
                code_send[par, lax.rem(k, 2), direction, h] = code
            for direction in going:
                for copy in ring_copies(u, k, direction, h):
                    copy.start()

    def finish(u):
        pair_copy_last(u).wait()
        wait_ring_sent(u, half - 1, half == 1)
        row_at = pl.multiple_of(lax.rem(u, slabs) * SUBLANES, SUBLANES)
        rows_at = pl.ds(row_at, SUBLANES)
        lanes = pl.ds(pl.multiple_of(lax.div(u, slabs) * LANES, LANES), LANES)
        for h in range(2):
            total = [
                parts_last[1, h, f] + pair_recv_last[ring_slot(u), h, f] for f in range(SUMS)
            ]
            for direction in range(2):
                if half > 1 or direction == h:
                    wait_ring(u, half - 1, direction, h)
                    earlier = received(u, half - 1, direction, h)
                    total = [a + b for a, b in zip(total, earlier)]
            packed, s1, q1, sb, qb = total
            count_first, count_both = counts(packed)
            first_mean = s1 / jnp.maximum(count_first, 1.0)
            first_var = (q1 - s1 * first_mean) / jnp.maximum(count_first - 1.0, 1.0)
            shift_sum = sb - first_mean * count_both
            shift_square = qb - first_mean * (sb + shift_sum)
            move = shift_sum / jnp.maximum(count_both, 1.0)
            final_var = (shift_square - shift_sum * move) / jnp.maximum(
                count_both - 1.0, 1.0
            )
            at = pl.ds(2 * h, 2)
            mean_out[0, at, rows_at, lanes] = first_mean
            mean_out[1, at, rows_at, lanes] = first_mean + move
            var_out[0, at, rows_at, lanes] = first_var
            var_out[1, at, rows_at, lanes] = final_var

    def advance(u, k):
        @pl.when(k == 0)
        def _():
            tick(u, 0, 0)

        if half > 1:

            @pl.when(k == 1)
            def _():
                tick(u, 1, 1)

        if half > 2:

            @pl.when(k > 1)
            def _():
                tick(u, k, 2)

        for i in range(units):

            @pl.when(jnp.logical_and(u == i, k + 1 < half))
            def _():
                partials(i, k + 1)

            @pl.when(jnp.logical_and(u == i, k + 1 == half))
            def _():
                partials_last(i)

    def arrive(a):
        for i in range(units):

            @pl.when(a == i)
            def _():
                wait_unit(i)
                partials(i, 0)

    def segment(a, outer):
        def step(k, middle):
            @pl.when(jnp.logical_and(k == lead - 1, a >= rings))
            def _():
                finish(a - rings)

            def ring(m, inner):
                r = rings - 1 - m
                u = a - r

                @pl.when(jnp.logical_and(k == 0, r == min(1, rings - 1)))
                def _():
                    arrive(a)

                @pl.when(jnp.logical_and(u >= 0, u < units))
                def _():
                    advance(u, r * lead + k)

                return inner

            return lax.fori_loop(0, rings, ring, middle)

        return lax.fori_loop(0, lead, step, outer)

    lax.fori_loop(0, units + rings, segment, 0)
    for u in range(units):
        wait_unit_sent(u)


def per_device(visit_tiles, warp_matrix, flux_scale, patch_lists, clip_bits):
    visits, blocks, rows, columns = visit_tiles.shape
    entries = visits * blocks
    xs = lax.axis_size("depth")
    skies = lax.axis_size("sky")
    zs = skies // CORES
    half = zs // 2
    share = rows // xs
    chunks = columns // LANES
    patches = PATCH_DEV * skies

    targets = patch_lists.reshape(entries, 1)
    named = targets == jnp.arange(patches, dtype=jnp.int32)[None, :]
    number = jnp.arange(entries, dtype=jnp.int32)[:, None]
    lowest = jnp.min(jnp.where(named, number, entries), axis=0)
    highest = jnp.max(jnp.where(named, number, -1), axis=0)
    table = jnp.stack([lowest, jnp.where(highest > lowest, highest, entries)])

    bits = clip_bits.reshape(entries, xs, chunks, LANES).transpose(1, 2, 0, 3)
    tiles = visit_tiles.reshape(visits, blocks * rows, columns)

    dims = (visits, blocks, rows, columns, xs, zs)
    out = jax.ShapeDtypeStruct((2, PATCH_DEV, share, columns), jnp.float32)
    any_spec = pl.BlockSpec(memory_space=pl.ANY)
    vmem_spec = pl.BlockSpec(memory_space=pltpu.VMEM)
    dma = pltpu.SemaphoreType.DMA
    slabs = share // SUBLANES
    units = chunks * slabs
    unit = (SUBLANES, LANES)
    sums = (SUMS, 2) + unit
    floats = (FLOATS, 2) + unit
    rings = min(RINGS, half)
    return pl.pallas_call(
        functools.partial(kernel_body, dims),
        out_shape=(out, out),
        in_specs=[
            any_spec,
            any_spec,
            pl.BlockSpec(memory_space=pltpu.SMEM),
            any_spec,
            any_spec,
        ],
        out_specs=(vmem_spec, vmem_spec),
        scratch_shapes=[
            pltpu.VMEM((visits, blocks * rows, columns), jnp.bfloat16),
            pltpu.VMEM((visits, columns, columns), jnp.bfloat16),
            pltpu.VMEM((xs, CAPACITY, patches), jnp.int32),
            pltpu.SMEM((xs, CAPACITY, patches), jnp.int32),
            *[pltpu.VMEM((xs, entries) + unit, jnp.bfloat16)] * units,
            *[pltpu.VMEM((xs, entries + 1) + unit, jnp.bfloat16)] * units,
            *[pltpu.VMEM((xs, entries + 8, LANES), jnp.int32)] * chunks,
            pltpu.VMEM((rings, 2, 2, 2) + sums, jnp.float32),
            pltpu.VMEM((2, 2) + sums, jnp.float32),
            pltpu.VMEM((rings, half, 2, 2) + sums, jnp.float32),
            pltpu.VMEM((rings, 2) + sums, jnp.float32),
            pltpu.VMEM((rings, 2, 2, 2) + floats, jnp.float32),
            pltpu.VMEM((rings, half, 2, 2) + floats, jnp.float32),
            pltpu.VMEM((rings, 2, 2, 2, 2) + unit, jnp.int32),
            pltpu.VMEM((rings, half, 2, 2, 2) + unit, jnp.int32),
            dma((visits, 2)),
            dma((2, xs)),
            dma((units + chunks,)),
            dma((units, visits, xs)),
            dma((units, visits, xs)),
            dma((chunks, xs)),
            dma((chunks, xs)),
            dma((rings + 1,)),
            dma((rings, half + 1)),
            dma((rings, 2, 2, 2, 2)),
            dma((rings, half, 2, 2, 2)),
        ],
        compiler_params=pltpu.CompilerParams(
            collective_id=0,
            has_side_effects=True,
            vmem_limit_bytes=66 * 1000 * 1000,
        ),
        name="coadd",
    )(tiles, warp_matrix, flux_scale, bits, table)


def solution(mesh):
    placed = (
        P(("tracts", "sky", "depth"), None, None, None),
        P(("tracts", "sky", "depth"), None, None),
        P(("tracts", "sky", "depth")),
        P(("tracts", "sky", "depth"), None),
        P(("tracts", "sky", "depth"), None, None, None),
    )
    return jax.shard_map(
        per_device,
        mesh=mesh,
        in_specs=placed,
        out_specs=(
            P(None, ("tracts", "sky"), "depth", None),
            P(None, ("tracts", "sky"), "depth", None),
        ),
        check_vma=False,
    )
```

```python
import functools

import jax
import jax.numpy as jnp
from jax import lax
from jax.experimental import pallas as pl
from jax.experimental.pallas import tpu as pltpu
from jax.sharding import PartitionSpec as P

PATCH_DEV = 4
CAPACITY = 2
CORES = 2
LANES = 128
SUBLANES = 8
SUMS = 5
FLOATS = 3
RINGS = 4
COUNT_UNIT = 4096.0
SHIFT_STEPS = 32767.0
RATIO_STEPS = 65535.0
TINY = 1e-37
MESH = pl.DeviceIdType.MESH


def kernel_body(
    dims,
    tiles_hbm,
    warp_hbm,
    flux,
    bits_hbm,
    table_hbm,
    mean_out,
    var_out,
    tiles,
    warp,
    table_v,
    table,
    *refs,
):
    visits, blocks, rows, columns, xs, zs = dims
    entries = visits * blocks
    share = rows // xs
    chunks = columns // LANES
    slabs = share // SUBLANES
    units = chunks * slabs
    half = zs // 2
    rings = min(RINGS, half)
    lead = -(-half // rings)
    x_send, x_recv = refs[:units], refs[units : 2 * units]
    bits = refs[2 * units : 2 * units + chunks]
    (
        parts,
        parts_last,
        pair_recv,
        pair_recv_last,
        ring_send,
        ring_recv,
        code_send,
        code_recv,
        load_sem,
        table_sem,
        own_sem,
        x_ssem,
        x_rsem,
        bits_ssem,
        bits_rsem,
        pair_ssem,
        pair_rsem,
        ring_ssem,
        ring_rsem,
    ) = refs[2 * units + chunks :]
    tract = lax.axis_index("tracts")
    sky = lax.axis_index("sky")
    x = lax.axis_index("depth")
    z, core = sky // CORES, lax.rem(sky, CORES)

    def x_peer(dx):
        return lax.rem(x + dx, xs)

    def z_peer(direction):
        step = 1 if direction == 0 else zs - 1
        return (tract, lax.rem(z + step, zs) * CORES + core, x)

    partner = (tract, z * CORES + (1 - core), x)

    barrier = pltpu.get_barrier_semaphore()
    greeted = [(tract, sky, x_peer(dx)) for dx in range(1, xs)]
    greeted += [z_peer(0), z_peer(1), partner]
    for device in greeted:
        pl.semaphore_signal(barrier, inc=1, device_id=device, device_id_type=MESH)

    def load_visit(v):
        return (
            pltpu.make_async_copy(tiles_hbm.at[v], tiles.at[v], load_sem.at[v, 0]),
            pltpu.make_async_copy(warp_hbm.at[v], warp.at[v], load_sem.at[v, 1]),
        )

    for v in range(visits):
        for copy in load_visit(v):
            copy.start()
    for s in range(xs):
        for u in range(units):
            x_recv[u][s, entries] = jnp.zeros((SUBLANES, LANES), jnp.bfloat16)
        for j in range(chunks):
            bits[j][s, pl.ds(entries, 8), :] = jnp.zeros((8, LANES), jnp.int32)
    pl.semaphore_wait(barrier, len(greeted))

    def table_copy(dx):
        return pltpu.make_async_remote_copy(
            src_ref=table_hbm,
            dst_ref=table_v.at[x],
            send_sem=table_sem.at[0, dx],
            recv_sem=table_sem.at[1, dx],
            device_id=(tract, sky, x_peer(dx)),
            device_id_type=MESH,
        )

    def bits_copy(j, dx):
        return pltpu.make_async_remote_copy(
            src_ref=bits_hbm.at[:, x_peer(dx), pl.ds(j * LANES, LANES)],
            dst_ref=bits[j].at[x, pl.ds(0, entries)],
            send_sem=bits_ssem.at[j, dx],
            recv_sem=bits_rsem.at[j, dx],
            device_id=(tract, sky, x_peer(dx)),
            device_id_type=MESH,
        )

    def x_copies(u, dx):
        pieces = visits if u == 0 else 1
        size = entries // pieces
        return [
            pltpu.make_async_remote_copy(
                src_ref=x_send[u].at[x_peer(dx), pl.ds(n * size, size)],
                dst_ref=x_recv[u].at[x, pl.ds(n * size, size)],
                send_sem=x_ssem.at[u, n, dx],
                recv_sem=x_rsem.at[u, n, dx],
                device_id=(tract, sky, x_peer(dx)),
                device_id_type=MESH,
            )
            for n in range(pieces)
        ]

    def own_bits(j):
        return pltpu.make_async_copy(
            bits_hbm.at[:, x, pl.ds(j * LANES, LANES)], bits[j].at[x, pl.ds(0, entries)], own_sem.at[units + j]
        )

    def own_rows(u):
        return pltpu.make_async_copy(
            x_send[u].at[x], x_recv[u].at[x, pl.ds(0, entries)], own_sem.at[u]
        )

    own_table = pltpu.make_async_copy(table_hbm, table_v.at[x], table_sem.at[0, 0])
    own_table.start()
    for dx in range(1, xs):
        table_copy(dx).start()

    group = 8
    for j in range(chunks):
        own_bits(j).start()
        for dx in range(1, xs):
            bits_copy(j, dx).start()
        for v in range(visits):
            if j == 0:
                for copy in load_visit(v):
                    copy.wait()
            weights = warp[v, :, pl.ds(j * LANES, LANES)]
            scale = flux[v]

            def multiply(n, carry):
                first = pl.multiple_of(n * (group * rows), group * rows)
                product = jnp.dot(
                    tiles[v, pl.ds(first, group * rows), :],
                    weights,
                    preferred_element_type=jnp.float32,
                )
                scaled = (product * scale).reshape(group, xs, slabs, SUBLANES, LANES)
                at = pl.ds(v * blocks + n * group, group)
                for d in range(xs):
                    for slab in range(slabs):
                        x_send[j * slabs + slab][d, at] = scaled[:, d, slab].astype(
                            jnp.bfloat16
                        )
                return carry

            lax.fori_loop(0, blocks // group, multiply, 0)
            if j == 0:
                for dx in range(1, xs):
                    x_copies(0, dx)[v].start()
        for u in range(j * slabs, (j + 1) * slabs):
            if u > 0:
                for dx in range(1, xs):
                    x_copies(u, dx)[0].start()
            own_rows(u).start()

    own_table.wait()
    for dx in range(1, xs):
        table_copy(dx).wait()
    to_scalar = pltpu.make_async_copy(table_v, table, table_sem.at[1, 0])
    to_scalar.start()
    to_scalar.wait()

    def wait_unit(u):
        if u % slabs == 0:
            own_bits(u // slabs).wait()
            for dx in range(1, xs):
                bits_copy(u // slabs, dx).wait_recv()
        own_rows(u).wait()
        for dx in range(1, xs):
            for copy in x_copies(u, dx):
                copy.wait_recv()

    def wait_unit_sent(u):
        for dx in range(1, xs):
            if u % slabs == 0:
                bits_copy(u // slabs, dx).wait_send()
            for copy in x_copies(u, dx):
                copy.wait_send()

    row = lax.broadcasted_iota(jnp.int32, (SUBLANES, LANES), 0)
    zero = jnp.zeros((SUBLANES, LANES), jnp.float32)

    def patch_sums(u, patch):
        j, slab = u // slabs, u % slabs
        mask_first = jnp.left_shift(jnp.int32(1), row + slab * SUBLANES)
        mask_both = jnp.bitwise_or(
            mask_first, jnp.left_shift(jnp.int32(1), row + (16 + slab * SUBLANES))
        )

        def source(s, sums):
            count, s1, q1, sb, qb = sums
            for r in range(CAPACITY):
                e = table[s, r, patch]
                sample = x_recv[u][s, e].astype(jnp.float32)
                word = bits[j][s, pl.ds(e, 1), :]
                first = jnp.bitwise_and(word, mask_first) != 0
                both = jnp.bitwise_and(word, mask_both) == mask_both
                kept = jnp.where(first, sample, 0.0)
                s1 = s1 + kept
                q1 = q1 + kept * kept
                kept = jnp.where(both, sample, 0.0)
                sb = sb + kept
                qb = qb + kept * kept
                count = count + jnp.where(
                    both, 1.0 + COUNT_UNIT, jnp.where(first, 1.0, 0.0)
                )
            return count, s1, q1, sb, qb

        return lax.fori_loop(0, xs, source, (zero,) * SUMS, unroll=True)

    def ring_slot(u):
        return lax.rem(u, rings)

    def pair_copy(u, k):
        return pltpu.make_async_remote_copy(
            src_ref=parts.at[ring_slot(u), 0],
            dst_ref=pair_recv.at[ring_slot(u), k],
            send_sem=pair_ssem.at[ring_slot(u)],
            recv_sem=pair_rsem.at[ring_slot(u), k],
            device_id=partner,
            device_id_type=MESH,
        )

    def pair_copy_last(u):
        return pltpu.make_async_remote_copy(
            src_ref=parts_last.at[0],
            dst_ref=pair_recv_last.at[ring_slot(u)],
            send_sem=pair_ssem.at[rings],
            recv_sem=pair_rsem.at[ring_slot(u), half],
            device_id=partner,
            device_id_type=MESH,
        )

    def store_group(dst, at, u, group):
        def two(h, carry):
            for q in range(2):
                sums = patch_sums(u, group * PATCH_DEV + 2 * h + q)
                for f, value in enumerate(sums):
                    dst[at + (h, f, q)] = value
            return carry

        lax.fori_loop(0, PATCH_DEV // 2, two, 0, unroll=True)

    def partials(u, k):
        if not (isinstance(k, int) and k == 0):
            pair_copy(u, k - 1).wait_send()
        forth = lax.rem(z + (half - k), zs) * CORES
        back = lax.rem(z + (half + k), zs) * CORES

        def one(n, carry):
            w, direction = jnp.right_shift(n, 1), jnp.bitwise_and(n, 1)
            which = jnp.where(w == 0, 1 - core, core)
            group = jnp.where(direction == 0, forth, back) + which
            store_group(parts, (ring_slot(u), w, direction), u, group)

            @pl.when(n == 1)
            def _():
                pair_copy(u, k).start()

            return carry

        lax.fori_loop(0, 2 * CORES, one, 0)

    def partials_last(u):
        pair_copy(u, half - 1).wait_send()
        if half > 1:
            wait_ring_sent(u, half - 2, half == 2)

        def one(w, carry):
            which = jnp.where(w == 0, 1 - core, core)
            store_group(parts_last, (w,), u, z * CORES + which)

            @pl.when(w == 0)
            def _():
                pair_copy_last(u).start()

            return carry

        lax.fori_loop(0, CORES, one, 0)

    def counts(packed):
        both = jnp.floor(packed * (1.0 / COUNT_UNIT))
        return packed - both * COUNT_UNIT, both

    def encode(packed, s1, q1, sb, qb):
        c1, cb = counts(packed)
        mean = s1 / jnp.maximum(c1, 1.0)
        mean_both = sb / jnp.maximum(cb, 1.0)
        m1 = jnp.maximum(q1 - s1 * mean, 0.0)
        mb = jnp.maximum(qb - sb * mean_both, 0.0)
        unit = lax.rsqrt(jnp.maximum(m1, TINY))
        shift = (mean_both - mean) * jnp.sqrt(cb) * unit
        shift = jnp.clip(shift, -1.0, 1.0) * SHIFT_STEPS
        ratio = jnp.minimum(mb * unit * unit, 1.0) * RATIO_STEPS
        code = jnp.bitwise_or(
            jnp.left_shift(jnp.floor(shift + 0.5).astype(jnp.int32), 16),
            jnp.floor(ratio + 0.5).astype(jnp.int32),
        )
        return (packed, s1, m1), code

    def decode(packed, s1, m1, code):
        c1, cb = counts(packed)
        mean = s1 / jnp.maximum(c1, 1.0)
        shift = jnp.right_shift(code, 16).astype(jnp.float32) * (1.0 / SHIFT_STEPS)
        ratio = jnp.bitwise_and(code, 65535).astype(jnp.float32) * (1.0 / RATIO_STEPS)
        spread = jnp.sqrt(m1) * lax.rsqrt(jnp.maximum(cb, 1.0))
        mean_both = mean + shift * spread
        sb = cb * mean_both
        return packed, s1, m1 + s1 * mean, sb, ratio * m1 + sb * mean_both

    def ring_copies(u, k, direction, h):
        par = ring_slot(u)
        return [
            pltpu.make_async_remote_copy(
                src_ref=send.at[par, lax.rem(k, 2), direction, h],
                dst_ref=recv.at[par, k, direction, h],
                send_sem=ring_ssem.at[par, lax.rem(k, 2), direction, h, kind],
                recv_sem=ring_rsem.at[par, k, direction, h, kind],
                device_id=z_peer(direction),
                device_id_type=MESH,
            )
            for kind, (send, recv) in enumerate(
                ((ring_send, ring_recv), (code_send, code_recv))
            )
        ]

    def wait_ring(u, k, direction, h):
        for copy in ring_copies(u, k, direction, h):
            copy.wait_recv()

    def wait_ring_sent(u, k, outset=False):
        for h in range(2):
            for direction in range(2):
                if not outset or direction == h:
                    for copy in ring_copies(u, k, direction, h):
                        copy.wait_send()

    def received(u, k, direction, h):
        at = (ring_slot(u), k, direction, h)
        return decode(*(ring_recv[at + (f,)] for f in range(FLOATS)), code_recv[at])

    def tick(u, k, stage):
        par = ring_slot(u)
        pair_copy(u, k).wait_recv()
        if stage > 1:

            @pl.when(k > 2)
            def _():
                wait_ring_sent(u, k - 2)

            @pl.when(k == 2)
            def _():
                wait_ring_sent(u, 0, True)

        for h in range(2):
            going = [d for d in range(2) if stage > 0 or d == h]
            coming = [d for d in range(2) if stage > 1 or (stage == 1 and d == h)]
            for direction in coming:
                wait_ring(u, k - 1, direction, h)
            ready = []
            for direction in going:
                sums = [
                    parts[par, 1, direction, h, f] + pair_recv[par, k, direction, h, f]
                    for f in range(SUMS)
                ]
                if direction in coming:
                    earlier = received(u, k - 1, direction, h)
                    sums = [a + b for a, b in zip(sums, earlier)]
                ready.append(encode(*sums))
            for direction, (floats, code) in zip(going, ready):
                for f in range(FLOATS):
                    ring_send[par, lax.rem(k, 2), direction, h, f] = floats[f]
                code_send[par, lax.rem(k, 2), direction, h] = code
            for direction in going:
                for copy in ring_copies(u, k, direction, h):
                    copy.start()

    def finish(u):
        pair_copy_last(u).wait()
        wait_ring_sent(u, half - 1, half == 1)
        row_at = pl.multiple_of(lax.rem(u, slabs) * SUBLANES, SUBLANES)
        rows_at = pl.ds(row_at, SUBLANES)
        lanes = pl.ds(pl.multiple_of(lax.div(u, slabs) * LANES, LANES), LANES)
        for h in range(2):
            total = [
                parts_last[1, h, f] + pair_recv_last[ring_slot(u), h, f] for f in range(SUMS)
            ]
            for direction in range(2):
                if half > 1 or direction == h:
                    wait_ring(u, half - 1, direction, h)
                    earlier = received(u, half - 1, direction, h)
                    total = [a + b for a, b in zip(total, earlier)]
            packed, s1, q1, sb, qb = total
            count_first, count_both = counts(packed)
            first_mean = s1 / jnp.maximum(count_first, 1.0)
            first_var = (q1 - s1 * first_mean) / jnp.maximum(count_first - 1.0, 1.0)
            shift_sum = sb - first_mean * count_both
            shift_square = qb - first_mean * (sb + shift_sum)
            move = shift_sum / jnp.maximum(count_both, 1.0)
            final_var = (shift_square - shift_sum * move) / jnp.maximum(
                count_both - 1.0, 1.0
            )
            at = pl.ds(2 * h, 2)
            mean_out[0, at, rows_at, lanes] = first_mean
            mean_out[1, at, rows_at, lanes] = first_mean + move
            var_out[0, at, rows_at, lanes] = first_var
            var_out[1, at, rows_at, lanes] = final_var

    def advance(u, k):
        @pl.when(k == 0)
        def _():
            tick(u, 0, 0)

        if half > 1:

            @pl.when(k == 1)
            def _():
                tick(u, 1, 1)

        if half > 2:

            @pl.when(k > 1)
            def _():
                tick(u, k, 2)

        for i in range(units):

            @pl.when(jnp.logical_and(u == i, k + 1 < half))
            def _():
                partials(i, k + 1)

            @pl.when(jnp.logical_and(u == i, k + 1 == half))
            def _():
                partials_last(i)

    def arrive(a):
        for i in range(units):

            @pl.when(a == i)
            def _():
                wait_unit(i)
                partials(i, 0)

    def segment(a, outer):
        def step(k, middle):
            @pl.when(jnp.logical_and(k == min(1, lead - 1), a >= rings))
            def _():
                finish(a - rings)

            def ring(m, inner):
                r = rings - 1 - m
                u = a - r

                @pl.when(jnp.logical_and(k == 0, r == min(1, rings - 1)))
                def _():
                    arrive(a)

                going = jnp.logical_and(u >= 0, u < units)

                @pl.when(jnp.logical_and(going, r * lead + k < half))
                def _():
                    advance(u, r * lead + k)

                return inner

            return lax.fori_loop(0, rings, ring, middle)

        return lax.fori_loop(0, lead, step, outer)

    lax.fori_loop(0, units + rings, segment, 0)
    for u in range(units):
        wait_unit_sent(u)


def per_device(visit_tiles, warp_matrix, flux_scale, patch_lists, clip_bits):
    visits, blocks, rows, columns = visit_tiles.shape
    entries = visits * blocks
    xs = lax.axis_size("depth")
    skies = lax.axis_size("sky")
    zs = skies // CORES
    half = zs // 2
    share = rows // xs
    chunks = columns // LANES
    patches = PATCH_DEV * skies

    targets = patch_lists.reshape(entries, 1)
    named = targets == jnp.arange(patches, dtype=jnp.int32)[None, :]
    number = jnp.arange(entries, dtype=jnp.int32)[:, None]
    lowest = jnp.min(jnp.where(named, number, entries), axis=0)
    highest = jnp.max(jnp.where(named, number, -1), axis=0)
    table = jnp.stack([lowest, jnp.where(highest > lowest, highest, entries)])

    bits = clip_bits.reshape(entries, xs, columns)
    tiles = visit_tiles.reshape(visits, blocks * rows, columns)

    dims = (visits, blocks, rows, columns, xs, zs)
    out = jax.ShapeDtypeStruct((2, PATCH_DEV, share, columns), jnp.float32)
    any_spec = pl.BlockSpec(memory_space=pl.ANY)
    vmem_spec = pl.BlockSpec(memory_space=pltpu.VMEM)
    dma = pltpu.SemaphoreType.DMA
    slabs = share // SUBLANES
    units = chunks * slabs
    unit = (SUBLANES, LANES)
    sums = (SUMS, 2) + unit
    floats = (FLOATS, 2) + unit
    rings = min(RINGS, half)
    return pl.pallas_call(
        functools.partial(kernel_body, dims),
        out_shape=(out, out),
        in_specs=[
            any_spec,
            any_spec,
            pl.BlockSpec(memory_space=pltpu.SMEM),
            any_spec,
            any_spec,
        ],
        out_specs=(vmem_spec, vmem_spec),
        scratch_shapes=[
            pltpu.VMEM((visits, blocks * rows, columns), jnp.bfloat16),
            pltpu.VMEM((visits, columns, columns), jnp.bfloat16),
            pltpu.VMEM((xs, CAPACITY, patches), jnp.int32),
            pltpu.SMEM((xs, CAPACITY, patches), jnp.int32),
            *[pltpu.VMEM((xs, entries) + unit, jnp.bfloat16)] * units,
            *[pltpu.VMEM((xs, entries + 1) + unit, jnp.bfloat16)] * units,
            *[pltpu.VMEM((xs, entries + 8, LANES), jnp.int32)] * chunks,
            pltpu.VMEM((rings, 2, 2, 2) + sums, jnp.float32),
            pltpu.VMEM((2, 2) + sums, jnp.float32),
            pltpu.VMEM((rings, half, 2, 2) + sums, jnp.float32),
            pltpu.VMEM((rings, 2) + sums, jnp.float32),
            pltpu.VMEM((rings, 2, 2, 2) + floats, jnp.float32),
            pltpu.VMEM((rings, half, 2, 2) + floats, jnp.float32),
            pltpu.VMEM((rings, 2, 2, 2, 2) + unit, jnp.int32),
            pltpu.VMEM((rings, half, 2, 2, 2) + unit, jnp.int32),
            dma((visits, 2)),
            dma((2, xs)),
            dma((units + chunks,)),
            dma((units, visits, xs)),
            dma((units, visits, xs)),
            dma((chunks, xs)),
            dma((chunks, xs)),
            dma((rings + 1,)),
            dma((rings, half + 1)),
            dma((rings, 2, 2, 2, 2)),
            dma((rings, half, 2, 2, 2)),
        ],
        compiler_params=pltpu.CompilerParams(
            collective_id=0,
            has_side_effects=True,
            vmem_limit_bytes=66 * 1000 * 1000,
        ),
        name="coadd",
    )(tiles, warp_matrix, flux_scale, bits, table)


def solution(mesh):
    placed = (
        P(("tracts", "sky", "depth"), None, None, None),
        P(("tracts", "sky", "depth"), None, None),
        P(("tracts", "sky", "depth")),
        P(("tracts", "sky", "depth"), None),
        P(("tracts", "sky", "depth"), None, None, None),
    )
    return jax.shard_map(
        per_device,
        mesh=mesh,
        in_specs=placed,
        out_specs=(
            P(None, ("tracts", "sky"), "depth", None),
            P(None, ("tracts", "sky"), "depth", None),
        ),
        check_vma=False,
    )
```
